32 devices in a mesh: mp: 8 (over z, x), dp: 4 (over y, core).
Axes of the slice: x: 2, y: 2, z: 4, core: 2. Of those that a mesh axis runs over, the one named last changes fastest.
Arguments:
- tables: bfloat16 [20, 16384, 128], P(None, 'mp'), may hold values from -3 to 3
- block_rows: int32 [2048, 128], P(('mp', 'dp')), may hold values from 0 to 2047
- block_slots: int32 [2048, 128], P(('mp', 'dp')), may hold values from 0 to 127
- block_table: int32 [2048], P(('mp', 'dp')), may hold values from 0 to 19
- block_peer: int32 [2048, 1], P(('mp', 'dp')), may hold values from 0 to 7; in each aligned block of 64 rows (0 to 63, 64 to 127, ...) at most 16 rows name the same one
- block_len: int32 [2048], P(('mp', 'dp')), may hold values from 1 to 128
- block_count: int32 [32], P(('mp', 'dp')), may hold values from 1 to 64, as said below
- cross_in: bfloat16 [4, 2560, 256], P(None, 'dp'), may hold values from -0.23632812 to 0.23632812
- cross_mix: bfloat16 [4, 256, 256], replicated, may hold values from -0.5625 to 0.5625
- cross_out: bfloat16 [4, 256, 2560], P(None, None, 'dp'), may hold values from -0.375 to 0.375
- cross_bias: float32 [4, 2560], replicated, may hold values from -3 to 3
- gate_weight: bfloat16 [4, 2560], replicated, may hold values from -0.47265625 to 0.47265625
Outputs:
- crossed: bfloat16 [4096, 2560], P(('mp', 'dp'))
The draws below stay inside these ranges and needn't reach their ends.
Inputs may be any that keep to these rules, and one draw needn't show every extreme that they name: `block_peer`: in the 64 blocks of one device no destination is named by more than 16 blocks, a bound that the blocks of some device reach. The live blocks of a device are its first block_count blocks; some device has exactly 64. Entries of a block at positions below its block_len are live. `block_rows`: A row index within the device's own shard of the table. `block_slots`: A sample of the destination device.
All inputs are finite; a program needn't handle non-finite values.
Results may differ from the reference program's by a relative error of at most 0.0059.
Values may be sent and summed in bfloat16 or wider, within the bound.
A program may use at most 128 MiB of HBM per device.

```python
import math
import jax
import jax.numpy as jnp
import numpy as np
from jax import lax

WIDTH = 128
TABLES = 20
ROWS_DEV = 2048
BLOCK = 128
NBLK = 64
B_DEV = 128
RANK = 256
EXPERTS = 4
D = 2560
CAP = 16
N_MP = 8
N_DP = 4


def draw_block_count(key, part):
    devices = N_MP * N_DP
    heavy = jax.random.randint(jax.random.fold_in(key, 11), (devices,), 0, 8) == 0
    high = jax.random.randint(jax.random.fold_in(key, 12), (devices,), NBLK // 2, NBLK + 1)
    low = jax.random.randint(jax.random.fold_in(key, 13), (devices,), max(1, NBLK // 8), NBLK // 2 + 1)
    counts = jnp.where(heavy, high, low)
    chosen = jax.random.randint(jax.random.fold_in(key, 14), (), 0, devices)
    return counts.at[chosen].set(NBLK).astype(jnp.int32)


def touch_ends(values, own_key, least, largest):
    extent = values.shape
    place = [jax.random.randint(jax.random.fold_in(own_key, axis), (), 0, extent[axis]) for axis in range(len(extent))]
    values = values.at[tuple(place)].set(least)
    longest = extent.index(max(extent))
    place[longest] = (place[longest] + 1) % extent[longest]
    return values.at[tuple(place)].set(largest)


def block_levels(key, extent, cuts, smallest, top_value):
    loudness = 1.0
    for dim, blocks in cuts:
        draws = jax.random.uniform(jax.random.fold_in(jax.random.fold_in(key, 6), dim), (blocks,), jnp.float32, smallest / len(cuts), top_value / len(cuts))
        loudness = loudness * jnp.repeat(jnp.exp(draws), extent[dim] // blocks).reshape((-1,) + (1,) * (len(extent) - 1 - dim))
    return loudness


def routed_block(key, own, number, rows, amount, top, bound, slope):
    order = jax.random.permutation(key, amount)
    packed, common = load_shares(amount, rows * top, bound, slope, True), load_shares(amount, rows * top, bound, slope, False)
    places = jnp.arange(amount)

    def named(tallies, rotation):
        used = int((tallies > 0).sum())
        fixed = max(1, used // 4)
        passed = fixed + (places - fixed + rotation * (used - fixed)) % max(1, amount - fixed)
        return jnp.zeros((amount,), jnp.int32).at[order[jnp.where(places < fixed, places, passed)]].set(jnp.asarray(tallies, jnp.int32))

    tallies = jnp.where(number % 4 == 0, named(packed, number // 4), named(common, number - number // 4 - 1))
    mixed = jax.random.permutation(jax.random.fold_in(own, 3), amount)
    donor, receiver = mixed[0:amount // 2 * 2:2], mixed[1:amount // 2 * 2:2]
    margin = jnp.minimum(tallies[donor] - 1, bound - tallies[receiver]) // 2
    margin = jnp.where((donor == order[0]) | (receiver == order[0]) | (tallies[receiver] == 0), 0, jnp.maximum(margin, 0))
    passed = jax.random.randint(jax.random.fold_in(own, 4), (amount // 2,), 0, 1 << 20) % (margin + 1)
    tallies = tallies.at[donor].add(-passed).at[receiver].add(passed)
    labels = jnp.searchsorted(jnp.cumsum(tallies), jnp.arange(rows * top), side="right").astype(jnp.int32)
    grid = labels.reshape(top, rows).T
    grid = grid[jax.random.permutation(jax.random.fold_in(own, 1), rows)]
    rotation = jax.random.randint(jax.random.fold_in(own, 2), (rows, 1), 0, top)
    return jnp.take_along_axis(grid, (jnp.arange(top)[None, :] + rotation) % top, axis=1)


def load_shares(count, total, reach, skew, full):
    weights = [(1 << 20) // math.isqrt(standing ** skew) + 1 for standing in range(1, count + 1)]
    largest = reach if full else min(reach, max(-(-total // count), total * weights[0] // sum(weights)))
    least = 1 if total - largest >= count - 1 else 0
    given, surplus = [largest] + [least] * (count - 1), total - largest - least * (count - 1)
    while surplus > 0:
        free = [i for i in range(1, count) if given[i] < largest] or [i for i in range(1, count) if given[i] < reach]
        whole, budget = sum([weights[i] for i in free]), surplus
        for i in free:
            extra = min(reach - given[i], max(1, budget * weights[i] // whole), surplus)
            given[i] = given[i] + extra
            surplus = surplus - extra
    return np.array(given)


def normal_values(stream_key, dims, deviation, limit, shards=(), kind=jnp.bfloat16):
    level = block_levels(stream_key, dims, shards, -0.22, 0.18) if shards else 1.0
    values = jax.random.normal(stream_key, dims, jnp.float32) * deviation * level
    return jnp.minimum(jnp.maximum(values, -limit), limit).astype(kind)


def setup_inputs(seed: int = 0) -> dict:
    key_list = jax.random.split(jax.random.key(seed), 13)
    tables = normal_values(key_list[0], (TABLES, ROWS_DEV * N_MP, WIDTH), 0.5, 3.0, ((1, 8),))
    block_rows = touch_ends(jax.random.randint(key_list[1], (N_MP * N_DP * NBLK, BLOCK), 0, ROWS_DEV), jax.random.fold_in(key_list[1], 1), 0, ROWS_DEV - 1).astype(jnp.int32)
    block_slots = touch_ends(jax.random.randint(key_list[2], (N_MP * N_DP * NBLK, BLOCK), 0, B_DEV), jax.random.fold_in(key_list[2], 1), 0, B_DEV - 1).astype(jnp.int32)
    block_table = touch_ends(jax.random.randint(key_list[3], (N_MP * N_DP * NBLK,), 0, TABLES), jax.random.fold_in(key_list[3], 1), 0, TABLES - 1).astype(jnp.int32)
    block_peer_keys = jax.random.split(jax.random.fold_in(key_list[4], 1), (N_MP * N_DP * NBLK) // NBLK)
    block_peer_turns = jax.random.permutation(jax.random.fold_in(key_list[4], 3), (N_MP * N_DP * NBLK) // NBLK)
    block_peer = jax.vmap(lambda own, number: routed_block(jax.random.fold_in(key_list[4], 2), own, number, NBLK, N_MP, 1, CAP, 2))(block_peer_keys, block_peer_turns).reshape((N_MP * N_DP * NBLK, 1))
    block_len = touch_ends(jax.random.randint(key_list[5], (N_MP * N_DP * NBLK,), 1, BLOCK + 1), jax.random.fold_in(key_list[5], 1), 1, BLOCK).astype(jnp.int32)
    block_count = draw_block_count(jax.random.fold_in(key_list[12], 71), 0)
    cross_in = normal_values(key_list[7], (EXPERTS, D, RANK), (2.0 / D ** 0.5), 0.23632812, ((1, 4),))
    cross_mix = normal_values(key_list[8], (EXPERTS, RANK, RANK), (1.5 / RANK ** 0.5), 0.5625)
    cross_out = normal_values(key_list[9], (EXPERTS, RANK, D), RANK ** -0.5, 0.375, ((2, 4),))
    cross_bias = normal_values(key_list[10], (EXPERTS, D), 0.5, 3.0, (), jnp.float32)
    gate_weight = normal_values(key_list[11], (EXPERTS, D), (4.0 / D ** 0.5), 0.47265625)
    return {"tables": tables, "block_rows": block_rows, "block_slots": block_slots, "block_table": block_table, "block_peer": block_peer, "block_len": block_len, "block_count": block_count, "cross_in": cross_in, "cross_mix": cross_mix, "cross_out": cross_out, "cross_bias": cross_bias, "gate_weight": gate_weight}


def reference(tables, block_rows, block_slots, block_table, block_peer, block_len, block_count, cross_in, cross_mix, cross_out, cross_bias, gate_weight):
    devices = N_MP * N_DP
    rows_all = block_rows.reshape(devices, NBLK, BLOCK)
    slots_all = block_slots.reshape(devices, NBLK, BLOCK)
    table_all = block_table.reshape(devices, NBLK)
    peer_all = block_peer.reshape(devices, NBLK)
    length_all = block_len.reshape(devices, NBLK)
    entries = jnp.arange(BLOCK, dtype=jnp.int32)
    blocks = jnp.arange(NBLK, dtype=jnp.int32)

    def one_device(index, total):
        shard = index // N_DP
        group = index % N_DP
        live = (blocks[:, None] < block_count[index]) & (entries[None, :] < length_all[index][:, None])
        table_ids = jnp.broadcast_to(table_all[index][:, None], (NBLK, BLOCK)).astype(jnp.int32)
        peer_ids = jnp.broadcast_to(peer_all[index][:, None], (NBLK, BLOCK)).astype(jnp.int32)
        row_ids = (rows_all[index] + shard * ROWS_DEV).astype(jnp.int32)
        values = tables[table_ids, row_ids].astype(jnp.float32) * live[:, :, None].astype(jnp.float32)
        partial_value = jnp.zeros((N_MP, TABLES, B_DEV, WIDTH), jnp.float32)
        partial_value = partial_value.at[peer_ids, table_ids, slots_all[index]].add(values)
        rounded = lax.optimization_barrier(partial_value.astype(jnp.bfloat16)).astype(jnp.float32)
        return total.at[:, group].add(rounded)

    total = lax.fori_loop(0, devices, one_device, jnp.zeros((N_MP, N_DP, TABLES, B_DEV, WIDTH), jnp.float32))
    embedded = total.transpose(0, 1, 3, 2, 4).reshape(devices * B_DEV, TABLES * WIDTH).astype(jnp.bfloat16)
    gate = jax.nn.sigmoid(jnp.dot(embedded, gate_weight.T, preferred_element_type=jnp.float32))
    weighted = jnp.zeros(embedded.shape, jnp.float32)
    for expert in range(EXPERTS):
        hidden = jnp.tanh(jnp.dot(embedded, cross_in[expert], preferred_element_type=jnp.float32)).astype(jnp.bfloat16)
        mixed = jnp.tanh(jnp.dot(hidden, cross_mix[expert], preferred_element_type=jnp.float32)).astype(jnp.bfloat16)
        expand = jnp.dot(mixed, cross_out[expert], preferred_element_type=jnp.float32) + cross_bias[expert][None, :]
        weighted = weighted + gate[:, expert][:, None] * expand
    base = embedded.astype(jnp.float32)
    return (base + base * weighted).astype(jnp.bfloat16)
```

```python
import functools

import jax
import jax.numpy as jnp
from jax import lax
from jax.experimental import pallas as pl
from jax.experimental.pallas import tpu as pltpu
from jax.sharding import PartitionSpec as P

B_DEV = 128
UNROLL = 4
STREAMS = 4
MESH = pl.DeviceIdType.MESH
VMEM_LIMIT = 67043328


def pool_kernel(
    unroll,
    count_ref,
    table_ref,
    peer_ref,
    len_ref,
    rows_ref,
    slots_ref,
    tables_ref,
    out_ref,
    acc,
    slot_of,
    key_of,
):
    table_count, rows_dev, width = tables_ref.shape
    total_blocks, block = rows_ref.shape
    tiles, samples, _ = out_ref.shape
    count = count_ref[0]

    def clear(i, carry):
        out_ref[i] = jnp.zeros((samples, width), jnp.bfloat16)
        slot_of[i] = -1
        return carry

    lax.fori_loop(0, tiles, clear, 0)

    lane = lax.broadcasted_iota(jnp.int32, (block, 128), 1)
    sample = lax.broadcasted_iota(jnp.int32, (samples, block), 0)
    entry = lax.broadcasted_iota(jnp.int32, (samples, block), 1)

    def group(g, used):
        made = []
        for u in range(unroll):
            b = g * unroll + u
            row = rows_ref[pl.ds(b, 1), :]
            slot = slots_ref[pl.ds(b, 1), :]
            table = table_ref[b]
            column = jnp.broadcast_to(row, (128, block)).T
            pick = jnp.concatenate(
                [
                    jnp.where(column == lane + c * 128, 1.0, 0.0).astype(jnp.bfloat16)
                    for c in range(rows_dev // 128)
                ],
                axis=1,
            )
            picked = jnp.dot(pick, tables_ref[table], preferred_element_type=jnp.float32)
            place = jnp.where((sample == slot) & (entry < len_ref[b]), 1.0, 0.0)
            made.append(
                jnp.dot(
                    place.astype(jnp.bfloat16),
                    picked.astype(jnp.bfloat16),
                    preferred_element_type=jnp.float32,
                )
            )
        for u in range(unroll):
            b = g * unroll + u
            key = peer_ref[b] * table_count + table_ref[b]
            live = b < count
            known = slot_of[key]
            first = known < 0
            at = jnp.where(live, jnp.where(first, used, known), total_blocks)
            acc[at] = jnp.where(first, made[u], acc[at] + made[u])
            slot_of[key] = jnp.where(live, at, known)
            key_of[at] = key
            used = used + jnp.where(live & first, 1, 0)
        return used

    used = lax.fori_loop(0, (count + unroll - 1) // unroll, group, 0)

    def flush(i, carry):
        out_ref[key_of[i]] = acc[i].astype(jnp.bfloat16)
        return carry

    lax.fori_loop(0, used, flush, 0)


def pool(peers, tables, block_rows, block_slots, block_table, block_peer, block_len, block_count):
    table_count, _, width = tables.shape
    total_blocks = block_rows.shape[0]
    tiles = peers * table_count
    unroll = UNROLL if total_blocks % UNROLL == 0 else 1
    smem = pl.BlockSpec(memory_space=pltpu.SMEM)
    vmem = pl.BlockSpec(memory_space=pltpu.VMEM)
    return pl.pallas_call(
        functools.partial(pool_kernel, unroll),
        out_shape=jax.ShapeDtypeStruct((tiles, B_DEV, width), jnp.bfloat16),
        in_specs=[smem] * 4 + [vmem] * 3,
        out_specs=vmem,
        scratch_shapes=[
            pltpu.VMEM((total_blocks + 1, B_DEV, width), jnp.float32),
            pltpu.SMEM((tiles,), jnp.int32),
            pltpu.SMEM((total_blocks + 1,), jnp.int32),
        ],
        compiler_params=pltpu.CompilerParams(vmem_limit_bytes=VMEM_LIMIT),
        name="pool",
    )(block_count, block_table, block_peer[:, 0], block_len, block_rows, block_slots, tables)


def cross_kernel(
    peers,
    share,
    partial_ref,
    in_ref,
    mix_ref,
    out_w_ref,
    bias_ref,
    gate_ref,
    result_ref,
    held,
    emb,
    win,
    wout,
    ring_send,
    ring_recv,
    w_send,
    w_recv,
    w_local,
):
    tiles, samples, width = partial_ref.shape
    table_count = tiles // peers
    part = table_count // STREAMS
    experts = mix_ref.shape[0]
    me = lax.axis_index("mp")
    half = peers // 2
    at = jnp.where(lax.rem(me, 2) == 0, lax.div(me, 2), peers - 1 - lax.div(me, 2))

    def member(position):
        position = lax.rem(position + 2 * peers, peers)
        return jnp.where(position < half, 2 * position, 2 * (peers - 1 - position) + 1)

    ahead, behind = member(at + 1), member(at - 1)

    barrier = pltpu.get_barrier_semaphore()
    greet = [{"mp": ahead}, {"mp": behind}]
    if share:
        d = lax.axis_index("dp")
        twin = d + 1 - 2 * lax.rem(d, 2)
        across = lax.rem(d + 2, 4)
        greet += [{"dp": twin}, {"dp": across}]
    for target in greet:
        pl.semaphore_signal(barrier, inc=1, device_id=target, device_id_type=MESH)
    pl.semaphore_wait(barrier, len(greet))

    def ring_copy(stream, source, step):
        target = ahead if stream % 2 == 0 else behind
        return pltpu.make_async_remote_copy(
            src_ref=source,
            dst_ref=held.at[step, stream],
            send_sem=ring_send.at[stream, step],
            recv_sem=ring_recv.at[stream, step],
            device_id={"mp": target},
            device_id_type=MESH,
        )

    def own_tiles(stream, distance):
        dest = member(at - distance if stream % 2 == 0 else at + distance)
        return pl.ds(dest * table_count + stream * part, part)

    for stream in range(STREAMS):
        ring_copy(stream, partial_ref.at[own_tiles(stream, 1)], 0).start()

    if share:

        def piece_refs(q, owner):
            if q < experts:
                return in_ref.at[q], win.at[owner, q]
            return out_w_ref.at[q - experts], wout.at[owner, q - experts]

        def w_copy(kind, q):
            if kind == 0:
                source, place = piece_refs(q, d)
                target = across
            elif kind == 1:
                source, place = piece_refs(q, d)
                target = twin
            else:
                _, place = piece_refs(q, across)
                source = place
                target = twin
            return pltpu.make_async_remote_copy(
                src_ref=source,
                dst_ref=place,
                send_sem=w_send.at[kind, q],
                recv_sem=w_recv.at[kind, q],
                device_id={"dp": target},
                device_id_type=MESH,
            )

        pieces = 2 * experts
        for kind in (0, 1):
            for q in range(pieces):
                w_copy(kind, q).start()
        local = []
        for q in range(pieces):
            source, place = piece_refs(q, d)
            local.append(pltpu.make_async_copy(source, place, w_local.at[q]))
            local[-1].start()

    def hop(step, last):
        for stream in range(STREAMS):
            ring_copy(stream, held.at[step, stream], step).wait_recv()
            mine = partial_ref[own_tiles(stream, step + 2)]
            total = held[step, stream].astype(jnp.float32) + mine.astype(jnp.float32)
            total = total.astype(jnp.bfloat16)
            if last:
                for i in range(part):
                    column = (stream * part + i) * width
                    emb[:, column : column + width] = total[i]
            else:
                held[step, stream] = total
                ring_copy(stream, held.at[step, stream], step + 1).start()

    if share:
        passed = 0
        for step in range(peers - 2):
            hop(step, False)
            if 1 <= step and passed < pieces:
                w_copy(0, passed).wait_recv()
                w_copy(2, passed).start()
                passed += 1
        hop(peers - 2, True)
        for q in range(passed, pieces):
            w_copy(0, q).wait_recv()
            w_copy(2, q).start()
        for q in range(pieces):
            local[q].wait()
    else:

        def turn(step, carry):
            hop(step, False)
            return carry

        lax.fori_loop(0, peers - 2, turn, 0)
        hop(peers - 2, True)

    owners = win.shape[0] if share else 1
    depth = in_ref.shape[1]
    columns = out_w_ref.shape[2]
    gate = jax.nn.sigmoid(
        lax.dot_general(
            emb[...], gate_ref[...], (((1,), (1,)), ((), ())), preferred_element_type=jnp.float32
        )
    )
    mixed = []
    for e in range(experts):
        if share:
            w_copy(1, e).wait_recv()
            w_copy(2, e).wait_recv()
        projected = jnp.zeros((samples, in_ref.shape[2]), jnp.float32)
        for o in range(owners):
            weight = win[o, e] if share else in_ref[e]
            projected += jnp.dot(
                emb[:, o * depth : (o + 1) * depth], weight, preferred_element_type=jnp.float32
            )
        hidden = jnp.tanh(projected).astype(jnp.bfloat16)
        mixed.append(
            jnp.tanh(
                jnp.dot(hidden, mix_ref[e], preferred_element_type=jnp.float32)
            ).astype(jnp.bfloat16)
        )
    if share:
        for e in range(experts):
            w_copy(1, experts + e).wait_recv()
            w_copy(2, experts + e).wait_recv()
    for o in range(owners):
        span = slice(o * columns, (o + 1) * columns)
        weighted = jnp.zeros((samples, columns), jnp.float32)
        for e in range(experts):
            weight = wout[o, e] if share else out_w_ref[e]
            grown = jnp.dot(mixed[e], weight, preferred_element_type=jnp.float32)
            weighted += gate[:, e : e + 1] * (grown + bias_ref[e : e + 1, span])
        base = emb[:, span].astype(jnp.float32)
        result_ref[:, span] = (base + base * weighted).astype(jnp.bfloat16)

    for stream in range(STREAMS):
        ring_copy(stream, partial_ref.at[own_tiles(stream, 1)], 0).wait_send()

    def sent(step, carry):
        for stream in range(STREAMS):
            ring_copy(stream, held.at[step - 1, stream], step).wait_send()
        return carry

    lax.fori_loop(1, peers - 1, sent, 0)
    if share:
        for kind in (0, 1, 2):
            for q in range(pieces):
                w_copy(kind, q).wait_send()


def cross(peers, groups, partial, cross_in, cross_mix, cross_out, cross_bias, gate_weight):
    tiles, samples, width = partial.shape
    table_count = tiles // peers
    experts = cross_in.shape[0]
    share = groups == 4 and cross_out.shape[2] % 128 == 0 and peers <= 8
    if not share:
        cross_in = lax.all_gather(cross_in, "dp", axis=1, tiled=True)
        cross_out = lax.all_gather(cross_out, "dp", axis=2, tiled=True)
        kept = (1, 8, 128), (1, 8, 128)
    else:
        kept = (groups, *cross_in.shape), (groups, *cross_out.shape)
    vmem = pl.BlockSpec(memory_space=pltpu.VMEM)
    return pl.pallas_call(
        functools.partial(cross_kernel, peers, share),
        out_shape=jax.ShapeDtypeStruct((samples, table_count * width), jnp.bfloat16),
        in_specs=[vmem] * 6,
        out_specs=vmem,
        scratch_shapes=[
            pltpu.VMEM((peers - 1, STREAMS, table_count // STREAMS, samples, width), jnp.bfloat16),
            pltpu.VMEM((samples, table_count * width), jnp.bfloat16),
            pltpu.VMEM(kept[0], jnp.bfloat16),
            pltpu.VMEM(kept[1], jnp.bfloat16),
            pltpu.SemaphoreType.DMA((STREAMS, peers - 1)),
            pltpu.SemaphoreType.DMA((STREAMS, peers - 1)),
            pltpu.SemaphoreType.DMA((3, 2 * experts)),
            pltpu.SemaphoreType.DMA((3, 2 * experts)),
            pltpu.SemaphoreType.DMA((2 * experts,)),
        ],
        compiler_params=pltpu.CompilerParams(
            collective_id=0, has_side_effects=True, vmem_limit_bytes=VMEM_LIMIT
        ),
        name="cross",
    )(partial, cross_in, cross_mix, cross_out, cross_bias, gate_weight)


def on_device(
    tables,
    block_rows,
    block_slots,
    block_table,
    block_peer,
    block_len,
    block_count,
    cross_in,
    cross_mix,
    cross_out,
    cross_bias,
    gate_weight,
):
    peers, groups = lax.axis_size("mp"), lax.axis_size("dp")
    partial = pool(
        peers, tables, block_rows, block_slots, block_table, block_peer, block_len, block_count
    )
    return cross(peers, groups, partial, cross_in, cross_mix, cross_out, cross_bias, gate_weight)


def solution(mesh):
    in_specs = (
        P(None, "mp", None),
        P(("mp", "dp"), None),
        P(("mp", "dp"), None),
        P(("mp", "dp")),
        P(("mp", "dp"), None),
        P(("mp", "dp")),
        P(("mp", "dp")),
        P(None, "dp", None),
        P(),
        P(None, None, "dp"),
        P(),
        P(),
    )
    out_specs = P(("mp", "dp"), None)
    return jax.shard_map(
        on_device, mesh=mesh, in_specs=in_specs, out_specs=out_specs, check_vma=False
    )
```

```python
import functools

import jax
import jax.numpy as jnp
from jax import lax
from jax.experimental import pallas as pl
from jax.experimental.pallas import tpu as pltpu
from jax.sharding import PartitionSpec as P

B_DEV = 128
UNROLL = 4
STREAMS = 4
MESH = pl.DeviceIdType.MESH
POOL_LIMIT = 30 << 20
CROSS_LIMIT = 34 << 20
VMEM_LIMIT = 67043328


def pool_kernel(
    unroll,
    count_ref,
    table_hbm,
    peer_hbm,
    len_hbm,
    rows_hbm,
    slots_hbm,
    tables_hbm,
    out_ref,
    table_ref,
    peer_ref,
    len_ref,
    rows_ref,
    slots_ref,
    tables_ref,
    acc,
    slot_of,
    key_of,
    ready,
    small_sem,
    table_sem,
):
    table_count, rows_dev, width = tables_ref.shape
    total_blocks, block = rows_ref.shape
    tiles, samples, _ = out_ref.shape
    pairs = (
        (table_hbm, table_ref),
        (peer_hbm, peer_ref),
        (len_hbm, len_ref),
        (rows_hbm, rows_ref),
        (slots_hbm, slots_ref),
    )
    small = [pltpu.make_async_copy(a, b, small_sem.at[i]) for i, (a, b) in enumerate(pairs)]
    for copy in small:
        copy.start()

    def table_copy(t):
        return pltpu.make_async_copy(tables_hbm.at[t], tables_ref.at[t], table_sem.at[t])

    for t in range(table_count):
        table_copy(t).start()
        ready[t] = 0

    def need(t):
        @pl.when(ready[t] == 0)
        def _():
            table_copy(t).wait()
            ready[t] = 1

    def clear(i, carry):
        out_ref[i] = jnp.zeros((samples, width), jnp.bfloat16)
        slot_of[i] = -1
        return carry

    lax.fori_loop(0, tiles, clear, 0)
    for copy in small:
        copy.wait()
    count = count_ref[0]

    lane = lax.broadcasted_iota(jnp.int32, (block, 128), 1)
    sample = lax.broadcasted_iota(jnp.int32, (samples, block), 0)
    entry = lax.broadcasted_iota(jnp.int32, (samples, block), 1)

    def group(g, used):
        made = []
        for u in range(unroll):
            need(table_ref[g * unroll + u])
        for u in range(unroll):
            b = g * unroll + u
            row = rows_ref[pl.ds(b, 1), :]
            slot = slots_ref[pl.ds(b, 1), :]
            table = table_ref[b]
            column = jnp.broadcast_to(row, (128, block)).T
            pick = jnp.concatenate(
                [
                    jnp.where(column == lane + c * 128, 1.0, 0.0).astype(jnp.bfloat16)
                    for c in range(rows_dev // 128)
                ],
                axis=1,
            )
            picked = jnp.dot(pick, tables_ref[table], preferred_element_type=jnp.float32)
            place = jnp.where((sample == slot) & (entry < len_ref[b]), 1.0, 0.0)
            made.append(
                jnp.dot(
                    place.astype(jnp.bfloat16),
                    picked.astype(jnp.bfloat16),
                    preferred_element_type=jnp.float32,
                )
            )
        for u in range(unroll):
            b = g * unroll + u
            key = peer_ref[b] * table_count + table_ref[b]
            live = b < count
            known = slot_of[key]
            first = known < 0
            at = jnp.where(live, jnp.where(first, used, known), total_blocks)
            acc[at] = jnp.where(first, made[u], acc[at] + made[u])
            slot_of[key] = jnp.where(live, at, known)
            key_of[at] = key
            used = used + jnp.where(live & first, 1, 0)
        return used

    used = lax.fori_loop(0, (count + unroll - 1) // unroll, group, 0)

    def flush(i, carry):
        out_ref[key_of[i]] = acc[i].astype(jnp.bfloat16)
        return carry

    lax.fori_loop(0, used, flush, 0)
    for t in range(table_count):
        need(t)


def pool(peers, tables, block_rows, block_slots, block_table, block_peer, block_len, block_count):
    table_count, _, width = tables.shape
    total_blocks = block_rows.shape[0]
    tiles = peers * table_count
    unroll = UNROLL if total_blocks % UNROLL == 0 else 1
    hbm = pl.BlockSpec(memory_space=pltpu.HBM)
    vmem = pl.BlockSpec(memory_space=pltpu.VMEM)
    return pl.pallas_call(
        functools.partial(pool_kernel, unroll),
        out_shape=jax.ShapeDtypeStruct((tiles, B_DEV, width), jnp.bfloat16),
        in_specs=[pl.BlockSpec(memory_space=pltpu.SMEM)] + [hbm] * 6,
        out_specs=vmem,
        scratch_shapes=[
            pltpu.SMEM((total_blocks,), jnp.int32),
            pltpu.SMEM((total_blocks,), jnp.int32),
            pltpu.SMEM((total_blocks,), jnp.int32),
            pltpu.VMEM(block_rows.shape, jnp.int32),
            pltpu.VMEM(block_slots.shape, jnp.int32),
            pltpu.VMEM(tables.shape, jnp.bfloat16),
            pltpu.VMEM((total_blocks + 1, B_DEV, width), jnp.float32),
            pltpu.SMEM((tiles,), jnp.int32),
            pltpu.SMEM((total_blocks + 1,), jnp.int32),
            pltpu.SMEM((table_count,), jnp.int32),
            pltpu.SemaphoreType.DMA((5,)),
            pltpu.SemaphoreType.DMA((table_count,)),
        ],
        compiler_params=pltpu.CompilerParams(
            vmem_limit_bytes=POOL_LIMIT if peers <= 8 else VMEM_LIMIT
        ),
        cost_estimate=pl.CostEstimate(
            flops=2 * total_blocks * B_DEV * tables.shape[1] * width,
            bytes_accessed=2 * tables.size + 2 * tiles * B_DEV * width,
            transcendentals=0,
        ),
        name="pool",
    )(
        block_count,
        *(
            pltpu.with_memory_space_constraint(x, pltpu.HBM)
            for x in (
                block_table,
                block_peer[:, 0],
                block_len,
                block_rows,
                block_slots,
                tables,
            )
        )
    )


def cross_kernel(
    peers,
    share,
    partial_ref,
    in_ref,
    far_ref,
    mix_ref,
    out_w_ref,
    bias_ref,
    gate_ref,
    result_ref,
    held,
    emb,
    win,
    wout,
    ring_send,
    ring_recv,
    w_send,
    w_recv,
    w_local,
):
    tiles, samples, width = partial_ref.shape
    table_count = tiles // peers
    part = table_count // STREAMS
    experts = mix_ref.shape[0]
    me = lax.axis_index("mp")
    half = peers // 2
    at = jnp.where(lax.rem(me, 2) == 0, lax.div(me, 2), peers - 1 - lax.div(me, 2))

    def member(position):
        position = lax.rem(position + 2 * peers, peers)
        return jnp.where(position < half, 2 * position, 2 * (peers - 1 - position) + 1)

    ahead, behind = member(at + 1), member(at - 1)

    barrier = pltpu.get_barrier_semaphore()
    greet = [{"mp": ahead}, {"mp": behind}]
    if share:
        d = lax.axis_index("dp")
        twin = d + 1 - 2 * lax.rem(d, 2)
        across = lax.rem(d + 2, 4)
        greet += [{"dp": twin}, {"dp": across}]
    for target in greet:
        pl.semaphore_signal(barrier, inc=1, device_id=target, device_id_type=MESH)
    pl.semaphore_wait(barrier, len(greet))

    def ring_copy(stream, source, step):
        target = ahead if stream % 2 == 0 else behind
        return pltpu.make_async_remote_copy(
            src_ref=source,
            dst_ref=held.at[step, stream],
            send_sem=ring_send.at[stream, step],
            recv_sem=ring_recv.at[stream, step],
            device_id={"mp": target},
            device_id_type=MESH,
        )

    def own_tiles(stream, distance):
        dest = member(at - distance if stream % 2 == 0 else at + distance)
        return pl.ds(dest * table_count + stream * part, part)

    for stream in range(STREAMS):
        ring_copy(stream, partial_ref.at[own_tiles(stream, 1)], 0).start()

    if share:

        def piece_refs(q, owner):
            if q < experts:
                return in_ref.at[q], win.at[owner, q]
            return out_w_ref.at[q - experts], wout.at[owner, q - experts]

        def w_copy(kind, q):
            if kind == 0:
                source, place = piece_refs(q, d)
                target = across
            elif kind == 1:
                source, place = piece_refs(q, d)
                target = twin
            else:
                _, place = piece_refs(q, across)
                source = far_ref.at[q] if q < experts else place
                target = twin
            return pltpu.make_async_remote_copy(
                src_ref=source,
                dst_ref=place,
                send_sem=w_send.at[kind, q],
                recv_sem=w_recv.at[kind, q],
                device_id={"dp": target},
                device_id_type=MESH,
            )

        pieces = 2 * experts
        for q in range(experts, pieces):
            w_copy(0, q).start()
        for q in range(experts):
            w_copy(2, q).start()
        for q in range(pieces):
            w_copy(1, q).start()
        local = []
        for q in range(pieces):
            source, place = piece_refs(q, d)
            local.append(pltpu.make_async_copy(source, place, w_local.at[q]))
            local[-1].start()
        for q in range(experts):
            _, place = piece_refs(q, across)
            local.append(pltpu.make_async_copy(far_ref.at[q], place, w_local.at[pieces + q]))
            local[-1].start()

    def hop(step, last):
        for stream in range(STREAMS):
            ring_copy(stream, held.at[step, stream], step).wait_recv()
            mine = partial_ref[own_tiles(stream, step + 2)]
            total = held[step, stream].astype(jnp.float32) + mine.astype(jnp.float32)
            total = total.astype(jnp.bfloat16)
            if last:
                for i in range(part):
                    column = (stream * part + i) * width
                    emb[:, column : column + width] = total[i]
            else:
                held[step, stream] = total
                ring_copy(stream, held.at[step, stream], step + 1).start()

    if share:
        passed = experts
        for step in range(peers - 2):
            hop(step, False)
            if 1 <= step and passed < pieces:
                w_copy(0, passed).wait_recv()
                w_copy(2, passed).start()
                passed += 1
        hop(peers - 2, True)
        for q in range(passed, pieces):
            w_copy(0, q).wait_recv()
            w_copy(2, q).start()
        for copy in local:
            copy.wait()
    else:

        def turn(step, carry):
            hop(step, False)
            return carry

        lax.fori_loop(0, peers - 2, turn, 0)
        hop(peers - 2, True)

    owners = win.shape[0] if share else 1
    depth = in_ref.shape[1]
    columns = out_w_ref.shape[2]
    gate = jax.nn.sigmoid(
        lax.dot_general(
            emb[...], gate_ref[...], (((1,), (1,)), ((), ())), preferred_element_type=jnp.float32
        )
    )
    mixed = []
    for e in range(experts):
        if share:
            w_copy(1, e).wait_recv()
            w_copy(2, e).wait_recv()
        projected = jnp.zeros((samples, in_ref.shape[2]), jnp.float32)
        for o in range(owners):
            weight = win[o, e] if share else in_ref[e]
            projected += jnp.dot(
                emb[:, o * depth : (o + 1) * depth], weight, preferred_element_type=jnp.float32
            )
        hidden = jnp.tanh(projected).astype(jnp.bfloat16)
        mixed.append(
            jnp.tanh(
                jnp.dot(hidden, mix_ref[e], preferred_element_type=jnp.float32)
            ).astype(jnp.bfloat16)
        )
    if share:
        for e in range(experts):
            w_copy(1, experts + e).wait_recv()
            w_copy(2, experts + e).wait_recv()
    for o in range(owners):
        span = slice(o * columns, (o + 1) * columns)
        weighted = jnp.zeros((samples, columns), jnp.float32)
        for e in range(experts):
            weight = wout[o, e] if share else out_w_ref[e]
            grown = jnp.dot(mixed[e], weight, preferred_element_type=jnp.float32)
            weighted += gate[:, e : e + 1] * (grown + bias_ref[e : e + 1, span])
        base = emb[:, span].astype(jnp.float32)
        result_ref[:, span] = (base + base * weighted).astype(jnp.bfloat16)

    for stream in range(STREAMS):
        ring_copy(stream, partial_ref.at[own_tiles(stream, 1)], 0).wait_send()

    def sent(step, carry):
        for stream in range(STREAMS):
            ring_copy(stream, held.at[step - 1, stream], step).wait_send()
        return carry

    lax.fori_loop(1, peers - 1, sent, 0)
    if share:
        for kind in (0, 1, 2):
            for q in range(experts if kind == 0 else 0, pieces):
                w_copy(kind, q).wait_send()


def shared(peers, groups, cross_out):
    return groups == 4 and cross_out.shape[2] % 128 == 0 and peers <= 8


def cross(peers, groups, partial, cross_in, far_in, cross_mix, cross_out, cross_bias, gate_weight):
    tiles, samples, width = partial.shape
    table_count = tiles // peers
    experts = cross_in.shape[0]
    share = shared(peers, groups, cross_out)
    if not share:
        cross_in = lax.all_gather(cross_in, "dp", axis=1, tiled=True)
        cross_out = lax.all_gather(cross_out, "dp", axis=2, tiled=True)
        kept = (1, 8, 128), (1, 8, 128)
    else:
        kept = (groups, *cross_in.shape), (groups, *cross_out.shape)
    vmem = pl.BlockSpec(memory_space=pltpu.VMEM)
    return pl.pallas_call(
        functools.partial(cross_kernel, peers, share),
        out_shape=jax.ShapeDtypeStruct((samples, table_count * width), jnp.bfloat16),
        in_specs=[vmem] * 7,
        out_specs=vmem,
        scratch_shapes=[
            pltpu.VMEM((peers - 1, STREAMS, table_count // STREAMS, samples, width), jnp.bfloat16),
            pltpu.VMEM((samples, table_count * width), jnp.bfloat16),
            pltpu.VMEM(kept[0], jnp.bfloat16),
            pltpu.VMEM(kept[1], jnp.bfloat16),
            pltpu.SemaphoreType.DMA((STREAMS, peers - 1)),
            pltpu.SemaphoreType.DMA((STREAMS, peers - 1)),
            pltpu.SemaphoreType.DMA((3, 2 * experts)),
            pltpu.SemaphoreType.DMA((3, 2 * experts)),
            pltpu.SemaphoreType.DMA((3 * experts,)),
        ],
        compiler_params=pltpu.CompilerParams(
            collective_id=0,
            has_side_effects=True,
            vmem_limit_bytes=CROSS_LIMIT if peers <= 8 else VMEM_LIMIT,
        ),
        name="cross",
    )(partial, cross_in, far_in, cross_mix, cross_out, cross_bias, gate_weight)


def on_device(
    tables,
    block_rows,
    block_slots,
    block_table,
    block_peer,
    block_len,
    block_count,
    cross_in,
    cross_mix,
    cross_out,
    cross_bias,
    gate_weight,
):
    peers, groups = lax.axis_size("mp"), lax.axis_size("dp")
    if shared(peers, groups, cross_out):
        far_in = lax.ppermute(cross_in, "dp", [(i, (i + 2) % groups) for i in range(groups)])
    else:
        far_in = jnp.zeros((1, 8, 128), jnp.bfloat16)
    partial = pool(
        peers, tables, block_rows, block_slots, block_table, block_peer, block_len, block_count
    )
    return cross(
        peers, groups, partial, cross_in, far_in, cross_mix, cross_out, cross_bias, gate_weight
    )


def solution(mesh):
    in_specs = (
        P(None, "mp", None),
        P(("mp", "dp"), None),
        P(("mp", "dp"), None),
        P(("mp", "dp")),
        P(("mp", "dp"), None),
        P(("mp", "dp")),
        P(("mp", "dp")),
        P(None, "dp", None),
        P(),
        P(None, None, "dp"),
        P(),
        P(),
    )
    out_specs = P(("mp", "dp"), None)
    return jax.shard_map(
        on_device, mesh=mesh, in_specs=in_specs, out_specs=out_specs, check_vma=False
    )
```

```python
import functools

import jax
import jax.numpy as jnp
from jax import lax
from jax.experimental import pallas as pl
from jax.experimental.pallas import tpu as pltpu
from jax.sharding import PartitionSpec as P

B_DEV = 128
UNROLL = 8
STREAMS = 4
MESH = pl.DeviceIdType.MESH
POOL_LIMIT = 30 << 20
CROSS_LIMIT = 34 << 20
VMEM_LIMIT = 67043328


def pool_kernel(
    unroll,
    count_ref,
    table_hbm,
    peer_hbm,
    len_hbm,
    rows_hbm,
    slots_hbm,
    tables_hbm,
    out_ref,
    table_ref,
    peer_ref,
    len_ref,
    rows_ref,
    slots_ref,
    tables_ref,
    acc,
    slot_of,
    key_of,
    ready,
    small_sem,
    table_sem,
):
    table_count, rows_dev, width = tables_ref.shape
    total_blocks, block = rows_ref.shape
    tiles, samples, _ = out_ref.shape
    pairs = (
        (table_hbm, table_ref),
        (peer_hbm, peer_ref),
        (len_hbm, len_ref),
        (rows_hbm, rows_ref),
        (slots_hbm, slots_ref),
    )
    small = [pltpu.make_async_copy(a, b, small_sem.at[i]) for i, (a, b) in enumerate(pairs)]
    for copy in small:
        copy.start()

    def table_copy(t):
        return pltpu.make_async_copy(tables_hbm.at[t], tables_ref.at[t], table_sem.at[t])

    for t in range(table_count):
        table_copy(t).start()
        ready[t] = 0

    def need(t):
        @pl.when(ready[t] == 0)
        def _():
            table_copy(t).wait()
            ready[t] = 1

    def clear(i, carry):
        out_ref[i] = jnp.zeros((samples, width), jnp.bfloat16)
        slot_of[i] = -1
        return carry

    lax.fori_loop(0, tiles, clear, 0)
    for copy in small:
        copy.wait()
    count = count_ref[0]

    lane = lax.broadcasted_iota(jnp.int32, (block, 128), 1)
    sample = lax.broadcasted_iota(jnp.int32, (samples, block), 0)
    entry = lax.broadcasted_iota(jnp.int32, (samples, block), 1)

    def group(g, used):
        made = []
        for u in range(unroll):
            need(table_ref[g * unroll + u])
        for u in range(unroll):
            b = g * unroll + u
            row = rows_ref[pl.ds(b, 1), :]
            slot = slots_ref[pl.ds(b, 1), :]
            table = table_ref[b]
            column = jnp.broadcast_to(row, (128, block)).T
            pick = jnp.concatenate(
                [
                    jnp.where(column == lane + c * 128, 1.0, 0.0).astype(jnp.bfloat16)
                    for c in range(rows_dev // 128)
                ],
                axis=1,
            )
            picked = jnp.dot(pick, tables_ref[table], preferred_element_type=jnp.float32)
            place = jnp.where((sample == slot) & (entry < len_ref[b]), 1.0, 0.0)
            made.append(
                jnp.dot(
                    place.astype(jnp.bfloat16),
                    picked.astype(jnp.bfloat16),
                    preferred_element_type=jnp.float32,
                )
            )
        for u in range(unroll):
            b = g * unroll + u
            key = peer_ref[b] * table_count + table_ref[b]
            live = b < count
            known = slot_of[key]
            first = known < 0
            at = jnp.where(live, jnp.where(first, used, known), total_blocks)
            acc[at] = jnp.where(first, made[u], acc[at] + made[u])
            slot_of[key] = jnp.where(live, at, known)
            key_of[at] = key
            used = used + jnp.where(live & first, 1, 0)
        return used

    used = lax.fori_loop(0, (count + unroll - 1) // unroll, group, 0)

    def flush(i, carry):
        out_ref[key_of[i]] = acc[i].astype(jnp.bfloat16)
        return carry

    lax.fori_loop(0, used, flush, 0)
    for t in range(table_count):
        need(t)


def pool(peers, tables, block_rows, block_slots, block_table, block_peer, block_len, block_count):
    table_count, _, width = tables.shape
    total_blocks = block_rows.shape[0]
    tiles = peers * table_count
    unroll = UNROLL if total_blocks % UNROLL == 0 else 1
    hbm = pl.BlockSpec(memory_space=pltpu.HBM)
    vmem = pl.BlockSpec(memory_space=pltpu.VMEM)
    return pl.pallas_call(
        functools.partial(pool_kernel, unroll),
        out_shape=jax.ShapeDtypeStruct((tiles, B_DEV, width), jnp.bfloat16),
        in_specs=[pl.BlockSpec(memory_space=pltpu.SMEM)] + [hbm] * 6,
        out_specs=vmem,
        scratch_shapes=[
            pltpu.SMEM((total_blocks,), jnp.int32),
            pltpu.SMEM((total_blocks,), jnp.int32),
            pltpu.SMEM((total_blocks,), jnp.int32),
            pltpu.VMEM(block_rows.shape, jnp.int32),
            pltpu.VMEM(block_slots.shape, jnp.int32),
            pltpu.VMEM(tables.shape, jnp.bfloat16),
            pltpu.VMEM((total_blocks + 1, B_DEV, width), jnp.float32),
            pltpu.SMEM((tiles,), jnp.int32),
            pltpu.SMEM((total_blocks + 1,), jnp.int32),
            pltpu.SMEM((table_count,), jnp.int32),
            pltpu.SemaphoreType.DMA((5,)),
            pltpu.SemaphoreType.DMA((table_count,)),
        ],
        compiler_params=pltpu.CompilerParams(
            vmem_limit_bytes=POOL_LIMIT if peers <= 8 else VMEM_LIMIT
        ),
        cost_estimate=pl.CostEstimate(
            flops=2 * total_blocks * B_DEV * tables.shape[1] * width,
            bytes_accessed=2 * tables.size + 2 * tiles * B_DEV * width,
            transcendentals=0,
        ),
        name="pool",
    )(
        block_count,
        *(
            pltpu.with_memory_space_constraint(x, pltpu.HBM)
            for x in (
                block_table,
                block_peer[:, 0],
                block_len,
                block_rows,
                block_slots,
                tables,
            )
        )
    )


def cross_kernel(
    peers,
    share,
    partial_ref,
    in_ref,
    far_ref,
    mix_ref,
    out_w_ref,
    bias_ref,
    gate_ref,
    result_ref,
    held,
    emb,
    win,
    wout,
    ring_send,
    ring_recv,
    w_send,
    w_recv,
    w_local,
):
    tiles, samples, width = partial_ref.shape
    table_count = tiles // peers
    part = table_count // STREAMS
    experts = mix_ref.shape[0]
    ahead_count = far_ref.shape[0]
    me = lax.axis_index("mp")
    half = peers // 2
    at = jnp.where(lax.rem(me, 2) == 0, lax.div(me, 2), peers - 1 - lax.div(me, 2))

    def member(position):
        position = lax.rem(position + 2 * peers, peers)
        return jnp.where(position < half, 2 * position, 2 * (peers - 1 - position) + 1)

    ahead, behind = member(at + 1), member(at - 1)

    barrier = pltpu.get_barrier_semaphore()
    greet = [{"mp": ahead}, {"mp": behind}]
    if share:
        d = lax.axis_index("dp")
        twin = d + 1 - 2 * lax.rem(d, 2)
        across = lax.rem(d + 2, 4)
        greet += [{"dp": twin}, {"dp": across}]
    for target in greet:
        pl.semaphore_signal(barrier, inc=1, device_id=target, device_id_type=MESH)
    pl.semaphore_wait(barrier, len(greet))

    def ring_copy(stream, source, step):
        target = ahead if stream % 2 == 0 else behind
        return pltpu.make_async_remote_copy(
            src_ref=source,
            dst_ref=held.at[step, stream],
            send_sem=ring_send.at[stream, step],
            recv_sem=ring_recv.at[stream, step],
            device_id={"mp": target},
            device_id_type=MESH,
        )

    def own_tiles(stream, distance):
        dest = member(at - distance if stream % 2 == 0 else at + distance)
        return pl.ds(dest * table_count + stream * part, part)

    for stream in range(STREAMS):
        ring_copy(stream, partial_ref.at[own_tiles(stream, 1)], 0).start()

    if share:

        def piece_refs(q, owner):
            if q < experts:
                return in_ref.at[q], win.at[owner, q]
            return out_w_ref.at[q - experts], wout.at[owner, q - experts]

        def w_copy(kind, q):
            if kind == 0:
                source, place = piece_refs(q, d)
                target = across
            elif kind == 1:
                source, place = piece_refs(q, d)
                target = twin
            else:
                _, place = piece_refs(q, across)
                source = far_ref.at[q] if q < ahead_count else place
                target = twin
            return pltpu.make_async_remote_copy(
                src_ref=source,
                dst_ref=place,
                send_sem=w_send.at[kind, q],
                recv_sem=w_recv.at[kind, q],
                device_id={"dp": target},
                device_id_type=MESH,
            )

        pieces = 2 * experts
        for q in range(ahead_count, pieces):
            w_copy(0, q).start()
        for q in range(ahead_count):
            w_copy(2, q).start()
        for q in range(pieces):
            w_copy(1, q).start()
        local = []
        for q in range(pieces):
            source, place = piece_refs(q, d)
            local.append(pltpu.make_async_copy(source, place, w_local.at[q]))
            local[-1].start()
        for q in range(ahead_count):
            _, place = piece_refs(q, across)
            local.append(pltpu.make_async_copy(far_ref.at[q], place, w_local.at[pieces + q]))
            local[-1].start()

    def hop(step, last):
        for stream in range(STREAMS):
            ring_copy(stream, held.at[step, stream], step).wait_recv()
            mine = partial_ref[own_tiles(stream, step + 2)]
            total = held[step, stream].astype(jnp.float32) + mine.astype(jnp.float32)
            total = total.astype(jnp.bfloat16)
            if last:
                for i in range(part):
                    column = (stream * part + i) * width
                    emb[:, column : column + width] = total[i]
            else:
                held[step, stream] = total
                ring_copy(stream, held.at[step, stream], step + 1).start()

    if share:
        passed = ahead_count
        for step in range(peers - 2):
            hop(step, False)
            if 1 <= step and passed < pieces:
                w_copy(0, passed).wait_recv()
                w_copy(2, passed).start()
                passed += 1
        hop(peers - 2, True)
        for q in range(passed, pieces):
            w_copy(0, q).wait_recv()
            w_copy(2, q).start()
        for copy in local:
            copy.wait()
    else:

        def turn(step, carry):
            hop(step, False)
            return carry

        lax.fori_loop(0, peers - 2, turn, 0)
        hop(peers - 2, True)

    owners = win.shape[0] if share else 1
    depth = in_ref.shape[1]
    columns = out_w_ref.shape[2]
    gate = jax.nn.sigmoid(
        lax.dot_general(
            emb[...], gate_ref[...], (((1,), (1,)), ((), ())), preferred_element_type=jnp.float32
        )
    )
    mixed = []
    for e in range(experts):
        if share:
            w_copy(1, e).wait_recv()
            w_copy(2, e).wait_recv()
        projected = jnp.zeros((samples, in_ref.shape[2]), jnp.float32)
        for o in range(owners):
            weight = win[o, e] if share else in_ref[e]
            projected += jnp.dot(
                emb[:, o * depth : (o + 1) * depth], weight, preferred_element_type=jnp.float32
            )
        hidden = jnp.tanh(projected).astype(jnp.bfloat16)
        mixed.append(
            jnp.tanh(
                jnp.dot(hidden, mix_ref[e], preferred_element_type=jnp.float32)
            ).astype(jnp.bfloat16)
        )
    if share:
        for e in range(experts):
            w_copy(1, experts + e).wait_recv()
            w_copy(2, experts + e).wait_recv()
    for o in range(owners):
        span = slice(o * columns, (o + 1) * columns)
        weighted = jnp.zeros((samples, columns), jnp.float32)
        for e in range(experts):
            weight = wout[o, e] if share else out_w_ref[e]
            grown = jnp.dot(mixed[e], weight, preferred_element_type=jnp.float32)
            weighted += gate[:, e : e + 1] * (grown + bias_ref[e : e + 1, span])
        base = emb[:, span].astype(jnp.float32)
        result_ref[:, span] = (base + base * weighted).astype(jnp.bfloat16)

    for stream in range(STREAMS):
        ring_copy(stream, partial_ref.at[own_tiles(stream, 1)], 0).wait_send()

    def sent(step, carry):
        for stream in range(STREAMS):
            ring_copy(stream, held.at[step - 1, stream], step).wait_send()
        return carry

    lax.fori_loop(1, peers - 1, sent, 0)
    if share:
        for kind in (0, 1, 2):
            for q in range(ahead_count if kind == 0 else 0, pieces):
                w_copy(kind, q).wait_send()


def shared(peers, groups, cross_out):
    return groups == 4 and cross_out.shape[2] % 128 == 0 and peers <= 8


def cross(peers, groups, partial, cross_in, far_in, cross_mix, cross_out, cross_bias, gate_weight):
    tiles, samples, width = partial.shape
    table_count = tiles // peers
    experts = cross_in.shape[0]
    share = shared(peers, groups, cross_out)
    if not share:
        cross_in = lax.all_gather(cross_in, "dp", axis=1, tiled=True)
        cross_out = lax.all_gather(cross_out, "dp", axis=2, tiled=True)
        kept = (1, 8, 128), (1, 8, 128)
    else:
        kept = (groups, *cross_in.shape), (groups, *cross_out.shape)
    vmem = pl.BlockSpec(memory_space=pltpu.VMEM)
    return pl.pallas_call(
        functools.partial(cross_kernel, peers, share),
        out_shape=jax.ShapeDtypeStruct((samples, table_count * width), jnp.bfloat16),
        in_specs=[vmem] * 7,
        out_specs=vmem,
        scratch_shapes=[
            pltpu.VMEM((peers - 1, STREAMS, table_count // STREAMS, samples, width), jnp.bfloat16),
            pltpu.VMEM((samples, table_count * width), jnp.bfloat16),
            pltpu.VMEM(kept[0], jnp.bfloat16),
            pltpu.VMEM(kept[1], jnp.bfloat16),
            pltpu.SemaphoreType.DMA((STREAMS, peers - 1)),
            pltpu.SemaphoreType.DMA((STREAMS, peers - 1)),
            pltpu.SemaphoreType.DMA((3, 2 * experts)),
            pltpu.SemaphoreType.DMA((3, 2 * experts)),
            pltpu.SemaphoreType.DMA((3 * experts,)),
        ],
        compiler_params=pltpu.CompilerParams(
            collective_id=0,
            has_side_effects=True,
            vmem_limit_bytes=CROSS_LIMIT if peers <= 8 else VMEM_LIMIT,
        ),
        name="cross",
    )(partial, cross_in, far_in, cross_mix, cross_out, cross_bias, gate_weight)


def on_device(
    tables,
    block_rows,
    block_slots,
    block_table,
    block_peer,
    block_len,
    block_count,
    cross_in,
    cross_mix,
    cross_out,
    cross_bias,
    gate_weight,
):
    peers, groups = lax.axis_size("mp"), lax.axis_size("dp")
    if shared(peers, groups, cross_out):
        far_in = lax.ppermute(cross_in[: cross_in.shape[0] - 1], "dp", [(i, (i + 2) % groups) for i in range(groups)])
    else:
        far_in = jnp.zeros((1, 8, 128), jnp.bfloat16)
    partial = pool(
        peers, tables, block_rows, block_slots, block_table, block_peer, block_len, block_count
    )
    return cross(
        peers, groups, partial, cross_in, far_in, cross_mix, cross_out, cross_bias, gate_weight
    )


def solution(mesh):
    in_specs = (
        P(None, "mp", None),
        P(("mp", "dp"), None),
        P(("mp", "dp"), None),
        P(("mp", "dp")),
        P(("mp", "dp"), None),
        P(("mp", "dp")),
        P(("mp", "dp")),
        P(None, "dp", None),
        P(),
        P(None, None, "dp"),
        P(),
        P(),
    )
    out_specs = P(("mp", "dp"), None)
    return jax.shard_map(
        on_device, mesh=mesh, in_specs=in_specs, out_specs=out_specs, check_vma=False
    )
```
